8 devices in a mesh: dp: 2 (over z, y), sp: 4 (over x, core).
Axes of the slice: x: 2, y: 2, z: 1, core: 2. Of those that a mesh axis runs over, the one named last changes fastest.
Arguments:
- hidden: bfloat16 [4096, 3584], P(('dp', 'sp')), parts along dimension 0
- grad_out: bfloat16 [4096, 3584], P(('dp', 'sp')), parts along dimension 0
- positions: int32 [4096], P(('dp', 'sp')), parts along dimension 0
- doc_ids: int32 [4096], P(('dp', 'sp')), parts along dimension 0
- w_q: bfloat16 [3584, 3584], replicated
- w_k: bfloat16 [3584, 512], replicated
- w_v: bfloat16 [3584, 512], replicated
- w_o: bfloat16 [3584, 3584], replicated
Outputs:
- output 1: bfloat16 [4096, 3584], P(('dp', 'sp')), parts along dimension 0
- output 2: bfloat16 [4096, 3584], P(('dp', 'sp')), parts along dimension 0
- output 3: float32 [7168, 3584], P('dp'), parts along dimension 0
- output 4: float32 [7168, 512], P('dp'), parts along dimension 0
- output 5: float32 [7168, 512], P('dp'), parts along dimension 0
- output 6: float32 [7168, 3584], P('dp'), parts along dimension 0
There are 2 independent parts. The reference program is written for one: setup_inputs(seed, part) draws one part's arguments, and reference() takes and returns one part's arrays. A program takes and returns all parts, laid end to end along the dimension named above; an argument that names none is the same for every part.
All inputs are finite; a program needn't handle non-finite values.
Results may differ from the reference program's by a relative error of at most 0.0106176.
Values are sent between devices in bfloat16 or wider.
A program may use at most 1 GiB of HBM per device.

```python
import jax
import jax.numpy as jnp
from jax import lax

D = 3584
HEADS = 28
KV_HEADS = 4
HEAD = 128
SEQ = 2048

ROPE_THETA = 500000.0
ROPE_FACTOR = 8.0
ROPE_LOW = 1.0
ROPE_HIGH = 4.0
ROPE_OLD_CTX = 8192.0
SCORE_LIMIT = 32 * 1024 * 1024
NEG_BIG = -1.0e30


def draw_layout(layout_key):
    cut_key, start_key = jax.random.split(layout_key)
    cut_points = jnp.sort(jax.random.randint(cut_key, (2,), SEQ // 8, SEQ - SEQ // 8))
    token_idx = jnp.arange(SEQ, dtype=jnp.int32)
    doc_ids = jnp.sum(token_idx[:, None] >= cut_points[None, :], axis=1).astype(jnp.int32)
    bounds = jnp.concatenate([jnp.zeros((1,), jnp.int32), cut_points.astype(jnp.int32)])
    starts = jax.random.randint(start_key, (3,), 0, SEQ)
    positions = (starts[doc_ids] + token_idx - bounds[doc_ids]).astype(jnp.int32)
    return positions, doc_ids


def setup_inputs(seed: int = 0, part: int = 0) -> dict:
    part_key = jax.random.fold_in(jax.random.key(seed), part)
    hid_key, grad_key, layout_key = jax.random.split(part_key, 3)
    weight_keys = jax.random.split(jax.random.key(seed + 1), 4)
    hidden = jax.random.normal(hid_key, (SEQ, D), jnp.float32).astype(jnp.bfloat16)
    grad_out = jax.random.normal(grad_key, (SEQ, D), jnp.float32).astype(jnp.bfloat16)
    positions, doc_ids = draw_layout(layout_key)
    in_scale = D ** -0.5
    w_q = (jax.random.normal(weight_keys[0], (D, HEADS * HEAD), jnp.float32) * in_scale).astype(jnp.bfloat16)
    w_k = (jax.random.normal(weight_keys[1], (D, KV_HEADS * HEAD), jnp.float32) * in_scale).astype(jnp.bfloat16)
    w_v = (jax.random.normal(weight_keys[2], (D, KV_HEADS * HEAD), jnp.float32) * in_scale).astype(jnp.bfloat16)
    w_o = (jax.random.normal(weight_keys[3], (HEADS * HEAD, D), jnp.float32) * (HEADS * HEAD) ** -0.5).astype(jnp.bfloat16)
    return {"hidden": hidden, "grad_out": grad_out, "positions": positions, "doc_ids": doc_ids, "w_q": w_q, "w_k": w_k, "w_v": w_v, "w_o": w_o}


def rope_freqs():
    half_idx = jnp.arange(HEAD // 2, dtype=jnp.float32)
    inv_freq = jnp.power(ROPE_THETA, -2.0 * half_idx / HEAD)
    wavelen = 2.0 * jnp.pi / inv_freq
    smooth = (ROPE_OLD_CTX / wavelen - ROPE_LOW) / (ROPE_HIGH - ROPE_LOW)
    mixed_freq = (1.0 - smooth) * inv_freq / ROPE_FACTOR + smooth * inv_freq
    scaled = jnp.where(wavelen > ROPE_OLD_CTX / ROPE_LOW, inv_freq / ROPE_FACTOR, mixed_freq)
    return jnp.where(wavelen < ROPE_OLD_CTX / ROPE_HIGH, inv_freq, scaled)


def rope_tables(pos_vec):
    angles = pos_vec.astype(jnp.float32)[:, None] * rope_freqs()[None, :]
    return jnp.cos(angles)[:, None, :], jnp.sin(angles)[:, None, :]


def rotate(values, cos_tab, sin_tab):
    half_dim = values.shape[-1] // 2
    first_half = values[..., :half_dim]
    second_half = values[..., half_dim:]
    return jnp.concatenate([first_half * cos_tab - second_half * sin_tab, second_half * cos_tab + first_half * sin_tab], axis=-1)


def block_rows(n_query, head_count, n_keys):
    block_len = n_query
    while block_len % 16 == 0 and head_count * block_len * n_keys > SCORE_LIMIT:
        block_len = block_len // 2
    return block_len


def block_probs(q_blk, k_all, pos_blk, doc_blk, pos_all, doc_all):
    scores = jnp.einsum("qhgd,shd->hgqs", q_blk, k_all) * HEAD ** -0.5
    allowed = (pos_all[None, :] <= pos_blk[:, None]) & (doc_all[None, :] == doc_blk[:, None])
    scores = jnp.where(allowed, scores, NEG_BIG)
    row_peak = jnp.max(scores, axis=-1, keepdims=True)
    exp_vals = jnp.exp(scores - row_peak)
    return exp_vals / jnp.sum(exp_vals, axis=-1, keepdims=True)


def reference(hidden, grad_out, positions, doc_ids, w_q, w_k, w_v, w_o):
    group_size = HEADS // KV_HEADS
    score_scale = HEAD ** -0.5
    cos_tab, sin_tab = rope_tables(positions)
    q_pre = jnp.dot(hidden, w_q, preferred_element_type=jnp.float32).reshape(SEQ, HEADS, HEAD)
    k_pre = jnp.dot(hidden, w_k, preferred_element_type=jnp.float32).reshape(SEQ, KV_HEADS, HEAD)
    v_pre = jnp.dot(hidden, w_v, preferred_element_type=jnp.float32).reshape(SEQ, KV_HEADS, HEAD)
    q_rot = rotate(q_pre, cos_tab, sin_tab).astype(jnp.bfloat16).astype(jnp.float32)
    k_rot = rotate(k_pre, cos_tab, sin_tab).astype(jnp.bfloat16).astype(jnp.float32)
    v_val = v_pre.astype(jnp.bfloat16).astype(jnp.float32)
    block_len = block_rows(SEQ, HEADS, SEQ)
    n_blocks = SEQ // block_len
    q_blocks = q_rot.reshape(n_blocks, block_len, KV_HEADS, group_size, HEAD)
    pos_blocks = positions.reshape(n_blocks, block_len)
    doc_blocks = doc_ids.reshape(n_blocks, block_len)

    def fwd_block(block_in):
        q_blk, pos_blk, doc_blk = block_in
        prob_f32 = block_probs(q_blk, k_rot, pos_blk, doc_blk, positions, doc_ids)
        prob_bf = prob_f32.astype(jnp.bfloat16).astype(jnp.float32)
        return jnp.einsum("hgqs,shd->qhgd", prob_bf, v_val).astype(jnp.bfloat16)

    context = lax.map(fwd_block, (q_blocks, pos_blocks, doc_blocks)).reshape(SEQ, HEADS * HEAD)
    attn_out = jnp.dot(context, w_o, preferred_element_type=jnp.float32).astype(jnp.bfloat16)

    d_ctx = jnp.dot(grad_out, w_o.T, preferred_element_type=jnp.float32).astype(jnp.bfloat16)
    grad_wo = jnp.dot(context.T, grad_out, preferred_element_type=jnp.float32)
    d_ctx_blocks = d_ctx.astype(jnp.float32).reshape(n_blocks, block_len, KV_HEADS, group_size, HEAD)

    def bwd_block(acc_pair, block_in):
        dk_acc, dv_acc = acc_pair
        q_blk, dctx_blk, pos_blk, doc_blk = block_in
        prob_f32 = block_probs(q_blk, k_rot, pos_blk, doc_blk, positions, doc_ids)
        prob_bf = prob_f32.astype(jnp.bfloat16).astype(jnp.float32)
        d_prob = jnp.einsum("qhgd,shd->hgqs", dctx_blk, v_val)
        row_dot = jnp.sum(prob_f32 * d_prob, axis=-1, keepdims=True)
        d_score = (prob_f32 * (d_prob - row_dot) * score_scale).astype(jnp.bfloat16).astype(jnp.float32)
        dq_blk = jnp.einsum("hgqs,shd->qhgd", d_score, k_rot).astype(jnp.bfloat16)
        dk_acc = dk_acc + jnp.einsum("hgqs,qhgd->shd", d_score, q_blk)
        dv_acc = dv_acc + jnp.einsum("hgqs,qhgd->shd", prob_bf, dctx_blk)
        return (dk_acc, dv_acc), dq_blk

    zero_acc = jnp.zeros((SEQ, KV_HEADS, HEAD), jnp.float32)
    (dk_acc, dv_acc), dq_blocks = lax.scan(bwd_block, (zero_acc, zero_acc), (q_blocks, d_ctx_blocks, pos_blocks, doc_blocks))
    dq_rot = dq_blocks.reshape(SEQ, HEADS, HEAD).astype(jnp.float32)
    dq_pre = rotate(dq_rot, cos_tab, -sin_tab).astype(jnp.bfloat16).reshape(SEQ, HEADS * HEAD)
    dk_rot = dk_acc.astype(jnp.bfloat16).astype(jnp.float32)
    dk_pre = rotate(dk_rot, cos_tab, -sin_tab).astype(jnp.bfloat16).reshape(SEQ, KV_HEADS * HEAD)
    dv_pre = dv_acc.astype(jnp.bfloat16).reshape(SEQ, KV_HEADS * HEAD)
    grad_hidden = (jnp.dot(dq_pre, w_q.T, preferred_element_type=jnp.float32) + jnp.dot(dk_pre, w_k.T, preferred_element_type=jnp.float32) + jnp.dot(dv_pre, w_v.T, preferred_element_type=jnp.float32)).astype(jnp.bfloat16)
    grad_wq = jnp.dot(hidden.T, dq_pre, preferred_element_type=jnp.float32)
    grad_wk = jnp.dot(hidden.T, dk_pre, preferred_element_type=jnp.float32)
    grad_wv = jnp.dot(hidden.T, dv_pre, preferred_element_type=jnp.float32)
    return attn_out, grad_hidden, grad_wq, grad_wk, grad_wv, grad_wo
```

```python
import functools

import jax
import jax.numpy as jnp
from jax import lax
from jax.experimental import pallas as pl
from jax.experimental.pallas import tpu as pltpu
from jax.sharding import PartitionSpec as P

HEAD_DIM = 128
ROPE_THETA = 500000.0
ROPE_FACTOR = 8.0
ROPE_LOW = 1.0
ROPE_HIGH = 4.0
ROPE_OLD_CTX = 8192.0
NEG_BIG = -1.0e30
LOG2E = 1.4426950408889634
BQ = 256
BK = 256
F32 = jnp.float32
BF16 = jnp.bfloat16
VMEM_LIMIT = 60 * 1024 * 1024


def rope_freqs():
    half_idx = jnp.arange(HEAD_DIM // 2, dtype=jnp.float32)
    inv_freq = jnp.power(ROPE_THETA, -2.0 * half_idx / HEAD_DIM)
    wavelen = 2.0 * jnp.pi / inv_freq
    smooth = (ROPE_OLD_CTX / wavelen - ROPE_LOW) / (ROPE_HIGH - ROPE_LOW)
    mixed_freq = (1.0 - smooth) * inv_freq / ROPE_FACTOR + smooth * inv_freq
    scaled = jnp.where(wavelen > ROPE_OLD_CTX / ROPE_LOW, inv_freq / ROPE_FACTOR, mixed_freq)
    return jnp.where(wavelen < ROPE_OLD_CTX / ROPE_HIGH, inv_freq, scaled)


def rope_tables(pos_vec):
    angles = pos_vec.astype(jnp.float32)[:, None] * rope_freqs()[None, :]
    cos_tab, sin_tab = jnp.cos(angles), jnp.sin(angles)
    return jnp.concatenate([cos_tab, cos_tab], 1), jnp.concatenate([-sin_tab, sin_tab], 1)


def rotate(values, cos_tab, sin_tab):
    return values * cos_tab + pltpu.roll(values, HEAD_DIM // 2, 1) * sin_tab


def rotate_back(values, cos_tab, sin_tab):
    return values * cos_tab - pltpu.roll(values, HEAD_DIM // 2, 1) * sin_tab


def dot_nn(lhs, rhs):
    return lax.dot_general(lhs, rhs, (((1,), (0,)), ((), ())), preferred_element_type=F32)


def dot_nt(lhs, rhs):
    return lax.dot_general(lhs, rhs, (((1,), (1,)), ((), ())), preferred_element_type=F32)


def dot_tn(lhs, rhs):
    return lax.dot_general(lhs, rhs, (((0,), (0,)), ((), ())), preferred_element_type=F32)


def params(n_grid):
    return pltpu.CompilerParams(dimension_semantics=("arbitrary",) * n_grid, vmem_limit_bytes=VMEM_LIMIT)


def cost(flops, nbytes):
    return pl.CostEstimate(flops=int(flops), bytes_accessed=int(nbytes), transcendentals=0)


def kv_kernel(core_ref, x_ref, wk_ref, wv_ref, cos_ref, sin_ref, out_ref):
    x = x_ref[...]
    k_acc = dot_nn(x, wk_ref[...])
    cos, sin = cos_ref[...], sin_ref[...]
    width = k_acc.shape[1]
    for h in range(width // HEAD_DIM):
        cols = slice(h * HEAD_DIM, (h + 1) * HEAD_DIM)
        out_ref[:, cols] = rotate(k_acc[:, cols], cos, sin).astype(BF16)
    out_ref[:, width:] = dot_nn(x, wv_ref[...]).astype(BF16)


def kv_proj(core, x, w_k, w_v, cos, sin):
    tokens, depth = x.shape
    width = w_k.shape[1] // 2
    rows = tokens // 2
    return pl.pallas_call(
        kv_kernel,
        grid_spec=pltpu.PrefetchScalarGridSpec(
            num_scalar_prefetch=1,
            grid=(2,),
            in_specs=[
                pl.BlockSpec((rows, depth), lambda r, c: (r, 0)),
                pl.BlockSpec((depth, width), lambda r, c: (0, c[0])),
                pl.BlockSpec((depth, width), lambda r, c: (0, c[0])),
                pl.BlockSpec((rows, HEAD_DIM), lambda r, c: (r, 0)),
                pl.BlockSpec((rows, HEAD_DIM), lambda r, c: (r, 0)),
            ],
            out_specs=pl.BlockSpec((rows, 2 * width), lambda r, c: (r, 0)),
        ),
        out_shape=jax.ShapeDtypeStruct((tokens, 2 * width), BF16),
        compiler_params=params(1),
        cost_estimate=cost(4 * tokens * depth * width, 2 * tokens * depth + 4 * depth * width),
        name="kv_proj",
    )(core, x, w_k, w_v, cos, sin)


def proj_kernel(n_x, transposed, rope, core_ref, *refs):
    w = refs[n_x][...]
    out_ref = refs[-1]
    for p in range(n_x):
        tokens = refs[p].shape[0]
        rows = slice(p * tokens, (p + 1) * tokens)
        acc = (dot_nt if transposed else dot_nn)(refs[p][...], w)
        if rope:
            cos, sin = refs[n_x + 1][rows, :], refs[n_x + 2][rows, :]
            for h in range(acc.shape[1] // HEAD_DIM):
                cols = slice(h * HEAD_DIM, (h + 1) * HEAD_DIM)
                out_ref[rows, cols] = rotate(acc[:, cols], cos, sin).astype(BF16)
        else:
            out_ref[rows, :] = acc.astype(BF16)


def head_proj(core, xs, w, transposed, tables, name):
    tokens, depth = xs[0].shape
    width = (w.shape[0] if transposed else w.shape[1]) // 2
    bn = 256
    steps = width // bn
    total = tokens * len(xs)
    in_specs = [pl.BlockSpec((tokens, depth), lambda n, c: (0, 0)) for _ in xs]
    if transposed:
        in_specs.append(pl.BlockSpec((bn, depth), lambda n, c: (c[0] * steps + n, 0)))
    else:
        in_specs.append(pl.BlockSpec((depth, bn), lambda n, c: (0, c[0] * steps + n)))
    for _ in tables:
        in_specs.append(pl.BlockSpec((total, HEAD_DIM), lambda n, c: (0, 0)))
    return pl.pallas_call(
        functools.partial(proj_kernel, len(xs), transposed, bool(tables)),
        grid_spec=pltpu.PrefetchScalarGridSpec(
            num_scalar_prefetch=1,
            grid=(steps,),
            in_specs=in_specs,
            out_specs=pl.BlockSpec((total, bn), lambda n, c: (0, n)),
        ),
        out_shape=jax.ShapeDtypeStruct((total, width), BF16),
        compiler_params=params(1),
        cost_estimate=cost(2 * total * depth * width, 2 * (total * depth + depth * width + total * width)),
        name=name,
    )(core, *xs, w, *tables)


def attn_kernel(last_phase, n_group, n_pieces, meta_ref, q_ref, dctx_ref, *refs):
    k_refs, v_refs = refs[:n_pieces], refs[n_pieces : 2 * n_pieces]
    refs = refs[2 * n_pieces :]
    rows_ref, cosq_ref, sinq_ref = refs[:3]
    refs = refs[3:]
    if last_phase:
        cosk_ref, sink_ref, dk_in_ref, dv_in_ref = refs[:4]
        refs = refs[4:]
    ctx_ref, dq_ref, dk_ref, dv_ref = refs[:4]
    k_all, v_all, q_stack, dctx_stack, s_buf, p_buf, prob_buf, ds_buf, ctx_acc, dq_acc, dk_acc, dv_acc = refs[4:]

    qb = pl.program_id(1)
    n_q = pl.num_programs(1)
    scale = HEAD_DIM**-0.5
    piece = k_refs[0].shape[0]
    per_piece = piece // BK
    me = meta_ref[0]
    heads = [slice(h * HEAD_DIM, (h + 1) * HEAD_DIM) for h in range(n_group)]
    cols = [slice(h * BQ, (h + 1) * BQ) for h in range(n_group)]

    @pl.when(qb == 0)
    def _():
        for p in range(n_pieces):
            k_all[p * piece : (p + 1) * piece, :] = k_refs[p][...]
            v_all[p * piece : (p + 1) * piece, :] = v_refs[p][...]
        if last_phase:
            dk_acc[...] = dk_in_ref[...]
            dv_acc[...] = dv_in_ref[...]
        else:
            dk_acc[...] = jnp.zeros_like(dk_acc)
            dv_acc[...] = jnp.zeros_like(dv_acc)

    for h in range(n_group):
        q_stack[cols[h], :] = q_ref[:, heads[h]]
        dctx_stack[cols[h], :] = dctx_ref[:, heads[h]]
    ctx_acc[...] = jnp.zeros_like(ctx_acc)
    dq_acc[...] = jnp.zeros_like(dq_acc)
    lo_row = rows_ref[0:1, :]
    idx_row = rows_ref[1:2, :]
    first = meta_ref[1 + qb]
    last = meta_ref[1 + n_q + qb]
    width = n_group * BQ

    def key_rows(g):
        local = (lax.div(g, per_piece) ^ me) * per_piece + lax.rem(g, per_piece)
        return pl.ds(pl.multiple_of(local * BK, BK), BK)

    def buf_rows(g):
        return pl.ds(pl.multiple_of((g - first) * BK, BK), BK)

    def scores(g, peak):
        keys, buf = key_rows(g), buf_rows(g)
        k_blk, v_blk = k_all[keys, :], v_all[keys, :]
        key_idx = g * BK + lax.broadcasted_iota(jnp.int32, (BK, BQ), 0)
        allowed = (key_idx >= lo_row) & (key_idx <= idx_row)
        peaks = []
        for h in range(n_group):
            s = jnp.where(allowed, dot_nt(k_blk, q_stack[cols[h], :]), NEG_BIG)
            s_buf[buf, cols[h]] = s
            peaks.append(jnp.maximum(peak[:, cols[h]], jnp.max(s, axis=0, keepdims=True)))
            p_buf[buf, cols[h]] = dot_nt(v_blk, dctx_stack[cols[h], :])
        return jnp.concatenate(peaks, axis=1)

    peak = lax.fori_loop(first, last, scores, jnp.full((1, width), NEG_BIG, F32))

    def weights(g, carry):
        total, row_dot = carry
        buf = buf_rows(g)
        totals, dots = [], []
        for h in range(n_group):
            e = jnp.exp2((s_buf[buf, cols[h]] - peak[:, cols[h]]) * (scale * LOG2E))
            s_buf[buf, cols[h]] = e
            totals.append(jnp.sum(e, axis=0, keepdims=True))
            dots.append(jnp.sum(e * p_buf[buf, cols[h]], axis=0, keepdims=True))
        return total + jnp.concatenate(totals, axis=1), row_dot + jnp.concatenate(dots, axis=1)

    zero_row = jnp.zeros((1, width), F32)
    total, row_dot = lax.fori_loop(first, last, weights, (zero_row, zero_row))
    inv = 1.0 / total
    row_dot = row_dot * inv

    def grads(g, carry):
        keys, buf = key_rows(g), buf_rows(g)
        k_blk, v_blk = k_all[keys, :], v_all[keys, :]
        for h in range(n_group):
            prob = s_buf[buf, cols[h]] * inv[:, cols[h]]
            d_score = (prob * (p_buf[buf, cols[h]] - row_dot[:, cols[h]]) * scale).astype(BF16)
            prob = prob.astype(BF16)
            prob_buf[:, cols[h]] = prob
            ds_buf[:, cols[h]] = d_score
            ctx_acc[cols[h], :] += dot_tn(prob, v_blk)
            dq_acc[cols[h], :] += dot_tn(d_score, k_blk)
        dv_acc[keys, :] += dot_nn(prob_buf[...], dctx_stack[...])
        dk_acc[keys, :] += dot_nn(ds_buf[...], q_stack[...])
        return carry

    lax.fori_loop(first, last, grads, 0)
    cosq, sinq = cosq_ref[...], sinq_ref[...]
    for h in range(n_group):
        ctx_ref[:, heads[h]] = ctx_acc[cols[h], :].astype(BF16)
        dq = dq_acc[cols[h], :].astype(BF16).astype(F32)
        dq_ref[:, heads[h]] = rotate_back(dq, cosq, sinq).astype(BF16)

    @pl.when(qb == n_q - 1)
    def _():
        if last_phase:
            dk = dk_acc[...].astype(BF16).astype(F32)
            dk_ref[...] = rotate_back(dk, cosk_ref[...], sink_ref[...]).astype(BF16)
            dv_ref[...] = dv_acc[...].astype(BF16)
        else:
            dk_ref[...] = dk_acc[...]
            dv_ref[...] = dv_acc[...]


def attention(meta, q, dctx, kvs, rows, tables_q, last, name):
    n_rows, width = q.shape
    n_pieces = len(kvs)
    piece = kvs[0].shape[0]
    n_kv = kvs[0].shape[1] // (2 * HEAD_DIM)
    n_group = width // HEAD_DIM // n_kv
    n_keys = piece * n_pieces
    group_blk = pl.BlockSpec((BQ, n_group * HEAD_DIM), lambda g, b, m: (b, g))
    key_blk = pl.BlockSpec((n_keys, HEAD_DIM), lambda g, b, m: (0, g))
    tab_blk = pl.BlockSpec((BQ, HEAD_DIM), lambda g, b, m: (b, 0))
    in_specs = [group_blk, group_blk]
    in_specs += [pl.BlockSpec((piece, HEAD_DIM), lambda g, b, m: (0, g)) for _ in kvs]
    in_specs += [pl.BlockSpec((piece, HEAD_DIM), lambda g, b, m: (0, n_kv + g)) for _ in kvs]
    in_specs += [pl.BlockSpec((2, BQ), lambda g, b, m: (0, b)), tab_blk, tab_blk]
    if last:
        full_k = pl.BlockSpec((n_keys, HEAD_DIM), lambda g, b, m: (0, 0))
        in_specs += [full_k, full_k, key_blk, key_blk]
    sum_type = BF16 if last else F32
    return pl.pallas_call(
        functools.partial(attn_kernel, bool(last), n_group, n_pieces),
        grid_spec=pltpu.PrefetchScalarGridSpec(
            num_scalar_prefetch=1,
            grid=(n_kv, n_rows // BQ),
            in_specs=in_specs,
            out_specs=[group_blk, group_blk, key_blk, key_blk],
            scratch_shapes=[
                pltpu.VMEM((n_keys, HEAD_DIM), BF16),
                pltpu.VMEM((n_keys, HEAD_DIM), BF16),
                pltpu.VMEM((n_group * BQ, HEAD_DIM), BF16),
                pltpu.VMEM((n_group * BQ, HEAD_DIM), BF16),
                pltpu.VMEM((n_keys, n_group * BQ), F32),
                pltpu.VMEM((n_keys, n_group * BQ), F32),
                pltpu.VMEM((BK, n_group * BQ), BF16),
                pltpu.VMEM((BK, n_group * BQ), BF16),
                pltpu.VMEM((n_group * BQ, HEAD_DIM), F32),
                pltpu.VMEM((n_group * BQ, HEAD_DIM), F32),
                pltpu.VMEM((n_keys, HEAD_DIM), F32),
                pltpu.VMEM((n_keys, HEAD_DIM), F32),
            ],
        ),
        out_shape=[
            jax.ShapeDtypeStruct((n_rows, width), BF16),
            jax.ShapeDtypeStruct((n_rows, width), BF16),
            jax.ShapeDtypeStruct((n_keys, n_kv * HEAD_DIM), sum_type),
            jax.ShapeDtypeStruct((n_keys, n_kv * HEAD_DIM), sum_type),
        ],
        compiler_params=params(2),
        cost_estimate=cost(12 * n_rows * n_keys * width, 8 * n_rows * width),
        name=name,
    )(meta, q, dctx, *kvs, *kvs, rows, *tables_q, *last)


def wgrad_q_kernel(has_acc, core_ref, x0_ref, x1_ref, mine_ref, other_ref, *refs):
    out_ref, lhs, lhs_swap = refs[-3:]
    half = pl.program_id(1)
    tokens = x0_ref.shape[0]

    @pl.when(half == 0)
    def _():
        first, second = x0_ref[...].T, x1_ref[...].T
        lhs[:, :tokens] = first
        lhs[:, tokens:] = second
        lhs_swap[:, :tokens] = second
        lhs_swap[:, tokens:] = first

    def fill(d_ref, lhs_ref):
        for n in range(0, d_ref.shape[1], 256):
            cols = slice(n, n + 256)
            acc = dot_nn(lhs_ref[...], d_ref[:, cols])
            out_ref[:, cols] = acc + refs[0][:, cols] if has_acc else acc

    @pl.when(half == 0)
    def _():
        fill(mine_ref, lhs)

    @pl.when(half == 1)
    def _():
        fill(other_ref, lhs_swap)


def wgrad_q(core, x0, x1, mine, other, acc, name):
    tokens, depth = x0.shape
    width = mine.shape[1]
    bm = 512
    x_blk = pl.BlockSpec((tokens, bm), lambda m, h, c: (0, m))
    d_blk = pl.BlockSpec((2 * tokens, width), lambda m, h, c: (0, 0))
    out_blk = pl.BlockSpec((bm, width), lambda m, h, c: (m, c[0] ^ h))
    return pl.pallas_call(
        functools.partial(wgrad_q_kernel, bool(acc)),
        grid_spec=pltpu.PrefetchScalarGridSpec(
            num_scalar_prefetch=1,
            grid=(depth // bm, 2),
            in_specs=[x_blk, x_blk, d_blk, d_blk] + [out_blk] * len(acc),
            out_specs=out_blk,
            scratch_shapes=[pltpu.VMEM((bm, 2 * tokens), BF16)] * 2,
        ),
        out_shape=jax.ShapeDtypeStruct((depth, 2 * width), F32),
        input_output_aliases={5: 0} if acc else {},
        compiler_params=params(2),
        cost_estimate=cost(8 * tokens * depth * width, 8 * depth * width),
        name=name,
    )(core, x0, x1, mine, other, *acc)


def wgrad_o_kernel(has_acc, core_ref, mine_ref, other_ref, g0_ref, g1_ref, *refs):
    out_ref, lhs, rhs = refs[-3:]
    m, n = pl.program_id(0), pl.program_id(1)
    tokens = g0_ref.shape[0]

    @pl.when((n == 0) & (m < 2))
    def _():
        lhs[...] = mine_ref[...].T

    @pl.when((n == 0) & (m >= 2))
    def _():
        lhs[:, :tokens] = other_ref[tokens:, :].T
        lhs[:, tokens:] = other_ref[:tokens, :].T

    rhs[:tokens, :] = g0_ref[...]
    rhs[tokens:, :] = g1_ref[...]
    for n in range(0, rhs.shape[1], 256):
        cols = slice(n, n + 256)
        acc = dot_nn(lhs[...], rhs[:, cols])
        out_ref[:, cols] = acc + refs[0][:, cols] if has_acc else acc


def wgrad_o(core, mine, other, g0, g1, acc, name):
    tokens, depth = g0.shape
    width = mine.shape[1]
    bm, bn = width // 2, 512
    mine_blk = pl.BlockSpec((2 * tokens, bm), lambda m, n, c: (0, jnp.minimum(m, 1)))
    other_blk = pl.BlockSpec((2 * tokens, bm), lambda m, n, c: (0, jnp.maximum(m - 2, 0)))
    g_blk = pl.BlockSpec((tokens, bn), lambda m, n, c: (0, n))
    out_blk = pl.BlockSpec((bm, bn), lambda m, n, c: ((c[0] ^ (m >> 1)) * 2 + (m & 1), n))
    return pl.pallas_call(
        functools.partial(wgrad_o_kernel, bool(acc)),
        grid_spec=pltpu.PrefetchScalarGridSpec(
            num_scalar_prefetch=1,
            grid=(4, depth // bn),
            in_specs=[mine_blk, other_blk, g_blk, g_blk] + [out_blk] * len(acc),
            out_specs=out_blk,
            scratch_shapes=[pltpu.VMEM((bm, 2 * tokens), BF16), pltpu.VMEM((2 * tokens, bn), BF16)],
        ),
        out_shape=jax.ShapeDtypeStruct((2 * width, depth), F32),
        input_output_aliases={5: 0} if acc else {},
        compiler_params=params(2),
        cost_estimate=cost(8 * tokens * depth * width, 8 * depth * width),
        name=name,
    )(core, mine, other, g0, g1, *acc)


def wgrad_kv_kernel(core_ref, x0, x1, x2, x3, dk_mine, dv_mine, dk_other, dv_other, wk_ref, wv_ref, lhs, lhs_swap):
    tokens = x0.shape[0]
    core = core_ref[0]
    for p, x_ref in enumerate((x0, x1, x2, x3)):
        turned = x_ref[...].T
        lhs[:, p * tokens : (p + 1) * tokens] = turned
        q = p ^ 1
        lhs_swap[:, q * tokens : (q + 1) * tokens] = turned
    width = dk_mine.shape[1]
    mine = pl.ds(pl.multiple_of(core * width, width), width)
    other = pl.ds(pl.multiple_of((1 - core) * width, width), width)
    wk_ref[:, mine] = dot_nn(lhs[...], dk_mine[...])
    wv_ref[:, mine] = dot_nn(lhs[...], dv_mine[...])
    wk_ref[:, other] = dot_nn(lhs_swap[...], dk_other[...])
    wv_ref[:, other] = dot_nn(lhs_swap[...], dv_other[...])


def wgrad_kv(core, xs, mine, other):
    tokens, depth = xs[0].shape
    width = mine[0].shape[1]
    bm = 512
    x_blk = pl.BlockSpec((tokens, bm), lambda m, c: (0, m))
    d_blk = pl.BlockSpec((4 * tokens, width), lambda m, c: (0, 0))
    out_blk = pl.BlockSpec((bm, 2 * width), lambda m, c: (m, 0))
    return pl.pallas_call(
        wgrad_kv_kernel,
        grid_spec=pltpu.PrefetchScalarGridSpec(
            num_scalar_prefetch=1,
            grid=(depth // bm,),
            in_specs=[x_blk] * 4 + [d_blk] * 4,
            out_specs=[out_blk, out_blk],
            scratch_shapes=[pltpu.VMEM((bm, 4 * tokens), BF16)] * 2,
        ),
        out_shape=[jax.ShapeDtypeStruct((depth, 2 * width), F32)] * 2,
        compiler_params=params(1),
        cost_estimate=cost(32 * tokens * depth * width, 8 * tokens * depth),
        name="wgrad_kv",
    )(core, *xs, *mine, *other)


def sum_kernel(n_terms, transposed, core_ref, *refs):
    dot = dot_nt if transposed else dot_nn
    total = dot(refs[0][...], refs[n_terms][...])
    for t in range(1, n_terms):
        total = total + dot(refs[t][...], refs[n_terms + t][...])
    refs[-1][...] = total.astype(BF16)


def sum_of_dots(core, terms, transposed, tokens, depth, name):
    bn = 512
    a_specs, w_specs = [], []
    flops = 0
    for a, row_block, w, other in terms:
        width = a.shape[1]
        flops += 2 * tokens * width * depth
        a_specs.append(pl.BlockSpec((tokens, width), lambda n, c, r=row_block: (r, 0)))
        if transposed:
            w_specs.append(pl.BlockSpec((bn, width), lambda n, c, o=other: (n, c[0] ^ o)))
        else:
            w_specs.append(pl.BlockSpec((width, bn), lambda n, c, o=other: (c[0] ^ o, n)))
    return pl.pallas_call(
        functools.partial(sum_kernel, len(terms), transposed),
        grid_spec=pltpu.PrefetchScalarGridSpec(
            num_scalar_prefetch=1,
            grid=(depth // bn,),
            in_specs=a_specs + w_specs,
            out_specs=pl.BlockSpec((tokens, bn), lambda n, c: (0, n)),
        ),
        out_shape=jax.ShapeDtypeStruct((tokens, depth), BF16),
        compiler_params=params(1),
        cost_estimate=cost(flops, flops // tokens),
        name=name,
    )(core, *[t[0] for t in terms], *[t[2] for t in terms])


def solution(mesh):
    sp_size = mesh.shape["sp"]

    def swap(value, bits):
        return lax.ppermute(value, "sp", [(s, s ^ bits) for s in range(sp_size)])

    def after(value, earlier):
        return lax.optimization_barrier((value, earlier))[0]

    def device_step(hidden, grad_out, positions, doc_ids, w_q, w_k, w_v, w_o):
        tokens, depth = hidden.shape
        me = lax.axis_index("sp").astype(jnp.int32)
        core = (me & 1).reshape(1)

        ids0 = jnp.stack([positions, doc_ids])
        ids = jnp.concatenate([ids0] + [swap(ids0, b) for b in (1, 2, 3)], axis=1)
        x0, g0 = hidden, grad_out
        x1 = swap(x0, 1)
        g1 = swap(g0, 1)

        cos, sin = rope_tables(ids[0])
        doc_all = ids[1]
        doc_start = jnp.sum((doc_all[None, :] < doc_all[:, None]).astype(jnp.int32), axis=1)
        token_idx = jnp.concatenate([(me ^ p) * tokens + jnp.arange(tokens, dtype=jnp.int32) for p in range(4)])
        rows = jnp.stack([doc_start, token_idx])
        first = doc_start[::BQ] // BK
        last = token_idx[BQ - 1 :: BQ] // BK + 1
        n_q = 2 * tokens // BQ

        def of_phase(phase):
            part = slice(2 * tokens * phase, 2 * tokens * (phase + 1))
            blk = slice(n_q * phase, n_q * (phase + 1))
            meta = jnp.concatenate([me.reshape(1), first[blk], last[blk]]).astype(jnp.int32)
            return meta, rows[:, part], (cos[part], sin[part])

        kv0 = kv_proj(core, x0, w_k, w_v, cos[:tokens], sin[:tokens])
        kv1 = kv_proj(core, after(x1, kv0), w_k, w_v, cos[tokens : 2 * tokens], sin[tokens : 2 * tokens])
        kv2, kv3 = swap(kv0, 2), swap(kv1, 2)
        x2 = swap(after(x0, kv1), 2)
        g2 = swap(after(g0, kv1), 2)

        meta_a, rows_a, tabs_a = of_phase(0)
        q_a = head_proj(core, (x0, after(x1, kv1)), w_q, False, tabs_a, "q_proj_own")
        dctx_a = head_proj(core, (g0, after(g1, q_a)), w_o, True, (), "dctx_own")
        kvs = (kv0, kv1, after(kv2, dctx_a), after(kv3, dctx_a))
        ctx_a, dq_a, dk_a, dv_a = attention(meta_a, q_a, dctx_a, kvs, rows_a, tabs_a, (), "attn_own")
        ctx_ao, dq_ao = swap(ctx_a, 1), swap(dq_a, 1)
        x2 = after(x2, ctx_a)
        x3 = swap(x2, 1)

        meta_b, rows_b, tabs_b = of_phase(1)
        q_b = head_proj(core, (x2, after(x3, ctx_a)), w_q, False, tabs_b, "q_proj_far")
        attn_out = sum_of_dots(core, [(ctx_a, 0, w_o, 0), (after(ctx_ao, q_b), 1, w_o, 1)], False, tokens, depth, "attn_out")
        grad_wo = wgrad_o(core, ctx_a, after(ctx_ao, attn_out), g0, g1, (), "wgrad_o_own")
        g2 = after(g2, attn_out)
        g3 = swap(g2, 1)
        grad_wq = wgrad_q(core, x0, x1, dq_a, after(dq_ao, grad_wo), (), "wgrad_q_own")

        dctx_b = head_proj(core, (g2, after(g3, grad_wq)), w_o, True, (), "dctx_far")
        ctx_b, dq_b, dk, dv = attention(meta_b, q_b, dctx_b, kvs, rows_b, tabs_b, (cos, sin, dk_a, dv_a), "attn_far")
        ctx_bo, dq_bo, dk_o, dv_o = swap(ctx_b, 1), swap(dq_b, 1), swap(dk, 1), swap(dv, 1)
        terms = [(dq_a, 0, w_q, 0), (dq_ao, 1, w_q, 1), (dk, 0, w_k, 0), (dk_o, 1, w_k, 1), (dv, 0, w_v, 0), (dv_o, 1, w_v, 1)]
        grad_hidden = sum_of_dots(core, terms, True, tokens, depth, "grad_hidden")
        grad_wk, grad_wv = wgrad_kv(core, (x0, x1, x2, x3), (dk, dv), (dk_o, after(dv_o, grad_hidden)))
        grad_wo = wgrad_o(core, ctx_b, after(ctx_bo, grad_wk), g2, g3, (grad_wo,), "wgrad_o_far")
        grad_wq = wgrad_q(core, x2, x3, dq_b, after(dq_bo, grad_wo), (grad_wq,), "wgrad_q_far")
        return attn_out, grad_hidden, grad_wq, grad_wk, grad_wv, grad_wo

    tok_spec = P(("dp", "sp"), None)
    vec_spec = P(("dp", "sp"))
    rep_spec = P(None, None)
    part_spec = P("dp", None)
    return jax.shard_map(device_step, mesh=mesh, in_specs=(tok_spec, tok_spec, vec_spec, vec_spec, rep_spec, rep_spec, rep_spec, rep_spec), out_specs=(tok_spec, tok_spec, part_spec, part_spec, part_spec, part_spec), check_vma=False)
```
